32 devices in a mesh: ctx: 4 (over x, core), exp: 8 (over z, y).
Axes of the slice: x: 2, y: 2, z: 4, core: 2. Of those that a mesh axis runs over, the one named last changes fastest.
Arguments:
- q_nope: bfloat16 [128, 128, 512], P('ctx', 'exp'), may hold values from -72 to 72
- q_rope: bfloat16 [128, 8192], P('ctx', 'exp'), may hold values from -6 to 6
- cache_keys: bfloat16 [576, 512], P(None, 'ctx'), may hold values from -6 to 6
- fresh_keys: bfloat16 [576, 128], P(None, 'ctx'), may hold values from -6 to 6
- block_order: int32 [8], replicated, may hold values from 0 to 7, each once
- w_uv: bfloat16 [128, 512, 128], P('exp'), may hold values from -0.25 to 0.25
- w_out: bfloat16 [16384, 7168], P('exp', 'ctx'), may hold values from -0.046875 to 0.046875
- residual: bfloat16 [128, 7168], P(('ctx', 'exp')), may hold values from -6 to 6
- norm_gain: float32 [7168], replicated, may hold values from 0.5 to 1.5
- router_weight: bfloat16 [7168, 16], replicated, may hold values from -0.0625 to 0.0625
- expert_ids: int32 [128, 8], P(('ctx', 'exp')), may hold values from 0 to 15, all different within a row; in each aligned block of 4 rows (0 to 3, 4 to 7, ...) at most 3 rows name the same one
- w_gate: bfloat16 [16, 7168, 2048], P('exp', None, 'ctx'), may hold values from -0.0625 to 0.0625
- w_up: bfloat16 [16, 7168, 2048], P('exp', None, 'ctx'), may hold values from -0.0625 to 0.0625
- w_down: bfloat16 [16, 2048, 7168], P('exp', 'ctx'), may hold values from -0.125 to 0.125
Outputs:
- layer_out: bfloat16 [128, 7168], P(('ctx', 'exp'))
The draws below stay inside these ranges and needn't reach their ends.
Inputs may be any that keep to these rules, and one draw needn't show every extreme that they name: A permutation: block j of the new tokens (16 rows) sits at positions 512 + block_order[j] * 16 onward. `expert_ids`: each row names 8 different experts; the 4 rows of one device name no expert more than 3 times, and in some aligned block one expert exactly 3 times.
All inputs are finite; a program needn't handle non-finite values.
Results may differ from the reference program's by a relative error of at most 0.012.
Values may be sent and summed in bfloat16 or wider, within the bound.
A program may use at most 128 MiB of HBM per device.

```python
import math
import jax
import jax.numpy as jnp
import numpy as np
from jax import lax

D = 7168
HEADS = 128
LAT = 512
ROPE = 64
QKD = 192
VHD = 128
FF = 2048
TOP = 8
EXPERTS = 16
TOK_DEV = 4
KD = 576
FFS = 512
CAP = 3
BLK = 16
NBLK = 8
NEWTOK = 128
CACHE = 512


def latent_cache(key):
    baseline = jax.random.normal(jax.random.fold_in(key, 101), (KD, CACHE), jnp.float32)
    return jnp.clip(baseline, -6.0, 6.0)


def draw_cache_keys(key, part):
    return latent_cache(key).astype(jnp.bfloat16)


def draw_q_nope(key, part):
    queries = jnp.clip(jax.random.normal(jax.random.fold_in(key, 202), (NEWTOK, HEADS, LAT), jnp.float32), -6.0, 6.0)
    return queries.astype(jnp.bfloat16)


def steps_of(rng, dims, cuts, low, top_value):
    loudness = 1.0
    for position, parts in cuts:
        steps = jax.random.uniform(jax.random.fold_in(jax.random.fold_in(rng, 6), position), (parts,), jnp.float32, low / len(cuts), top_value / len(cuts))
        loudness = loudness * jnp.repeat(jnp.exp(steps), dims[position] // parts).reshape((-1,) + (1,) * (len(dims) - 1 - position))
    return loudness


def shared_out(own_key, own, number, rows, amount, top, limit, skew):
    sequence = jax.random.permutation(own_key, amount)
    crowded, common = load_shares(amount, rows * top, limit, skew, True), load_shares(amount, rows * top, limit, skew, False)
    places = jnp.arange(amount)

    def named(tallies, rotation):
        used = int((tallies > 0).sum())
        fixed = max(1, used // 4)
        moved = fixed + (places - fixed + rotation * (used - fixed)) % max(1, amount - fixed)
        return jnp.zeros((amount,), jnp.int32).at[sequence[jnp.where(places < fixed, places, moved)]].set(jnp.asarray(tallies, jnp.int32))

    tallies = jnp.where(number % 4 == 0, named(crowded, number // 4), named(common, number - number // 4 - 1))
    mixed = jax.random.permutation(jax.random.fold_in(own, 3), amount)
    source_of, sink = mixed[0:amount // 2 * 2:2], mixed[1:amount // 2 * 2:2]
    room = jnp.minimum(tallies[source_of] - 1, limit - tallies[sink]) // 2
    room = jnp.where((source_of == sequence[0]) | (sink == sequence[0]) | (tallies[sink] == 0), 0, jnp.maximum(room, 0))
    moved = jax.random.randint(jax.random.fold_in(own, 4), (amount // 2,), 0, 1 << 20) % (room + 1)
    tallies = tallies.at[source_of].add(-moved).at[sink].add(moved)
    items = jnp.searchsorted(jnp.cumsum(tallies), jnp.arange(rows * top), side="right").astype(jnp.int32)
    table = items.reshape(top, rows).T
    table = table[jax.random.permutation(jax.random.fold_in(own, 1), rows)]
    rotation = jax.random.randint(jax.random.fold_in(own, 2), (rows, 1), 0, top)
    return jnp.take_along_axis(table, (jnp.arange(top)[None, :] + rotation) % top, axis=1)


def load_shares(count, total, bound, slope, full):
    loads = [(1 << 20) // math.isqrt(grade ** slope) + 1 for grade in range(1, count + 1)]
    largest = bound if full else min(bound, max(-(-total // count), total * loads[0] // sum(loads)))
    least = 1 if total - largest >= count - 1 else 0
    given, spare = [largest] + [least] * (count - 1), total - largest - least * (count - 1)
    while spare > 0:
        candidates = [i for i in range(1, count) if given[i] < largest] or [i for i in range(1, count) if given[i] < bound]
        pool, remaining = sum([loads[i] for i in candidates]), spare
        for i in candidates:
            extra = min(bound - given[i], max(1, remaining * loads[i] // pool), spare)
            given[i] = given[i] + extra
            spare = spare - extra
    return np.array(given)


def centred(stream_key, dims, width, most, cuts=(), kind=jnp.bfloat16):
    values = jax.random.normal(stream_key, dims, jnp.float32) * width
    if len(cuts) > 0:
        values = steps_of(stream_key, dims, cuts, -0.22, 0.18) * values
    return jnp.clip(values, min=-most, max=most).astype(kind)


def setup_inputs(seed: int = 0) -> dict:
    key_of = jax.random.split(jax.random.key(seed), 15)
    q_nope = draw_q_nope(jax.random.fold_in(key_of[14], 71), 0)
    q_rope = centred(key_of[1], (NEWTOK, HEADS * ROPE), 1.0, 6.0, ((0, 4), (1, 8)))
    cache_keys = draw_cache_keys(jax.random.fold_in(key_of[14], 71), 0)
    fresh_keys = centred(key_of[3], (KD, NEWTOK), 1.0, 6.0, ((1, 4),))
    block_order = jax.random.permutation(key_of[4], NBLK).astype(jnp.int32)
    w_uv = centred(key_of[5], (HEADS, LAT, VHD), LAT ** -0.5, 0.25, ((0, 8),))
    w_out = centred(key_of[6], (HEADS * VHD, D), (HEADS * VHD) ** -0.5, 0.046875, ((0, 8), (1, 4)))
    residual = centred(key_of[7], (NEWTOK, D), 1.0, 6.0, ((0, 32),))
    norm_gain = jnp.clip(1.0 + 0.1 * jax.random.normal(key_of[8], (D,), jnp.float32), 0.5, 1.5)
    router_weight = centred(key_of[9], (D, EXPERTS), D ** -0.5, 0.0625)
    expert_ids_keys = jax.random.split(jax.random.fold_in(key_of[10], 1), NEWTOK // TOK_DEV)
    expert_ids_turns = jax.random.permutation(jax.random.fold_in(key_of[10], 3), NEWTOK // TOK_DEV)
    expert_ids = jax.vmap(lambda own, number: shared_out(jax.random.fold_in(key_of[10], 2), own, number, TOK_DEV, EXPERTS, TOP, CAP, 2))(expert_ids_keys, expert_ids_turns).reshape((NEWTOK, TOP))
    w_gate = centred(key_of[11], (EXPERTS, D, FF), D ** -0.5, 0.0625, ((0, 8), (2, 4)))
    w_up = centred(key_of[12], (EXPERTS, D, FF), D ** -0.5, 0.0625, ((0, 8), (2, 4)))
    w_down = centred(key_of[13], (EXPERTS, FF, D), FF ** -0.5, 0.125, ((0, 8), (1, 4)))
    return dict(q_nope=q_nope, q_rope=q_rope, cache_keys=cache_keys, fresh_keys=fresh_keys, block_order=block_order, w_uv=w_uv, w_out=w_out, residual=residual, norm_gain=norm_gain, router_weight=router_weight, expert_ids=expert_ids, w_gate=w_gate, w_up=w_up, w_down=w_down)


ROUTE_SCALE = 2.5
NORM_EPS = 1e-06

def block_position(row_index, block_order):
    blocks = row_index // BLK
    lookup = blocks[:, None] == jnp.arange(NBLK, dtype=jnp.int32)[None, :]
    leading = lax.optimization_barrier(jnp.sum(jnp.where(lookup, block_order[None, :], 0), axis=1))
    return (leading * BLK + row_index % BLK).astype(jnp.int32)

def reference(q_nope, q_rope, cache_keys, fresh_keys, block_order, w_uv, w_out, residual, norm_gain, router_weight, expert_ids, w_gate, w_up, w_down):
    keys = jnp.concatenate([cache_keys, fresh_keys], axis=1)
    query_pos = block_position(jnp.arange(NEWTOK, dtype=jnp.int32), block_order)
    key_pos = jnp.concatenate([jnp.full((CACHE,), -1, jnp.int32), query_pos])
    visible = key_pos[None, :] <= query_pos[:, None]
    scale = 1.0 / math.sqrt(QKD)
    latent_keys = keys[:LAT]
    rotary_keys = keys[LAT:]

    def one_head(inputs):
        query_lat, query_pe, w_head = inputs
        first_dot = jnp.dot(query_lat, latent_keys, preferred_element_type=jnp.float32)
        second_dot = jnp.dot(query_pe, rotary_keys, preferred_element_type=jnp.float32)
        scores = jnp.where(visible, (first_dot + second_dot) * scale, -jnp.inf)
        row_max = lax.optimization_barrier(jnp.max(scores, axis=1, keepdims=True))
        exponent = jnp.exp(scores - row_max)
        row_sum = lax.optimization_barrier(jnp.sum(exponent, axis=1, keepdims=True))
        latent = lax.dot_general(exponent.astype(jnp.bfloat16), latent_keys, (((1,), (1,)), ((), ())), preferred_element_type=jnp.float32) / row_sum
        return jnp.dot(latent, w_head.astype(jnp.float32), precision=lax.Precision.HIGHEST).astype(jnp.bfloat16)
    head_inputs = (jnp.transpose(q_nope, (1, 0, 2)), jnp.transpose(q_rope.reshape(NEWTOK, HEADS, ROPE), (1, 0, 2)), w_uv)
    head_out = lax.map(one_head, head_inputs)
    head_out = jnp.transpose(head_out, (1, 0, 2)).reshape(NEWTOK, HEADS * VHD)
    attention = jnp.dot(head_out, w_out, preferred_element_type=jnp.float32).astype(jnp.bfloat16)
    hidden = residual.astype(jnp.float32) + attention.astype(jnp.float32)
    mean_square = lax.optimization_barrier(jnp.mean(hidden * hidden, axis=1, keepdims=True))
    normed = (hidden * lax.rsqrt(mean_square + NORM_EPS) * norm_gain).astype(jnp.bfloat16)
    affinity = jax.nn.sigmoid(jnp.dot(normed, router_weight, preferred_element_type=jnp.float32))
    chosen = jnp.take_along_axis(affinity, expert_ids, axis=1)
    route = ROUTE_SCALE * chosen / lax.optimization_barrier(jnp.sum(chosen, axis=1, keepdims=True))
    onehot = expert_ids[:, :, None] == jnp.arange(EXPERTS, dtype=jnp.int32)[None, None, :]
    mixing = lax.optimization_barrier(jnp.sum(jnp.where(onehot, route[:, :, None], 0.0), axis=1))

    def one_expert(running, inputs):
        gate_matrix, up_matrix, down_matrix, mix_column = inputs
        gate = jnp.dot(normed, gate_matrix, preferred_element_type=jnp.float32)
        upward = jnp.dot(normed, up_matrix, preferred_element_type=jnp.float32)
        act = (jax.nn.silu(gate) * upward).astype(jnp.bfloat16)
        act_blocks = jnp.transpose(act.reshape(NEWTOK, FF // FFS, FFS), (1, 0, 2))
        down_blocks = down_matrix.reshape(FF // FFS, FFS, D)

        def add_block(accum, pair):
            block_out = jnp.dot(pair[0], pair[1], preferred_element_type=jnp.float32).astype(jnp.bfloat16)
            block_out = lax.optimization_barrier(block_out)
            return (accum + block_out.astype(jnp.float32), None)
        summed, ignored = lax.scan(add_block, jnp.zeros((NEWTOK, D), jnp.float32), (act_blocks, down_blocks))
        expert_out = lax.optimization_barrier(summed.astype(jnp.bfloat16)).astype(jnp.float32)
        return (running + mix_column[:, None] * expert_out, None)
    mixture, ignored = lax.scan(one_expert, jnp.zeros((NEWTOK, D), jnp.float32), (w_gate, w_up, w_down, mixing.T))
    return (hidden + mixture).astype(jnp.bfloat16)
```

```python
import functools
import math

import jax
import jax.numpy as jnp
from jax import lax
from jax.experimental import pallas as pl
from jax.experimental.pallas import tpu as pltpu
from jax.sharding import PartitionSpec as P

QKD = 192
VMEM_BYTES = 48 * 1024 * 1024

ROUTE_SCALE = 2.5
NORM_EPS = 1e-06


def block_position(row_index, block_order, block_rows):
    blocks = row_index // block_rows
    lookup = blocks[:, None] == jnp.arange(block_order.shape[0], dtype=jnp.int32)[None, :]
    leading = jnp.sum(jnp.where(lookup, block_order[None, :], 0), axis=1)
    return leading * block_rows + row_index % block_rows


def attend(query_lat, query_pe, keys, visible):
    row_count, head_count, latent_width = query_lat.shape
    key_count = keys.shape[1]
    pe_width = query_pe.shape[1] // head_count
    first_dot = jnp.dot(
        query_lat.reshape(row_count * head_count, latent_width),
        keys[:latent_width],
        preferred_element_type=jnp.float32,
    )
    second_dot = jnp.dot(
        query_pe.reshape(row_count * head_count, pe_width),
        keys[latent_width:],
        preferred_element_type=jnp.float32,
    )
    scores = ((first_dot + second_dot) * (1.0 / math.sqrt(QKD))).reshape(
        row_count, head_count, key_count
    )
    scores = jnp.where(visible[:, None, :], scores, -jnp.inf)
    row_max = jnp.max(scores, axis=2)
    exponent = jnp.exp(scores - row_max[:, :, None])
    row_sum = jnp.sum(exponent, axis=2)
    weights = exponent.astype(jnp.bfloat16).reshape(row_count * head_count, key_count)
    latent = lax.dot_general(
        weights, keys[:latent_width], (((1,), (1,)), ((), ())), preferred_element_type=jnp.float32
    )
    return (row_max, row_sum, latent.reshape(row_count, head_count, latent_width))


def remote(src, dst, send, recv, target):
    return pltpu.make_async_remote_copy(
        src_ref=src,
        dst_ref=dst,
        send_sem=send,
        recv_sem=recv,
        device_id=target,
        device_id_type=pl.DeviceIdType.MESH,
    )


def place():
    ctx_count, exp_count = lax.axis_size("ctx"), lax.axis_size("exp")
    ctx, exp = lax.axis_index("ctx"), lax.axis_index("exp")
    return ctx_count // 2, exp_count, ctx, exp, ctx // 2, ctx % 2


def start_gather(src, out, send, recv):
    chips, _, ctx, exp, chip, core = place()
    flights = []
    for k in range(chips):
        peer = ctx + 1 - 2 * core if k == 0 else (chip + k) % chips * 2 + core
        copy = remote(src, out.at[ctx], send.at[0, k], recv.at[0, k], (peer, exp))
        copy.start()
        flights.append(copy)
    return flights


def finish_gather(out, flights, send, recv):
    chips, _, ctx, exp, chip, core = place()
    relayed = []
    for k in range(1, chips):
        flights[k].wait_recv()
        origin = (chip + chips - k) % chips * 2 + core
        copy = remote(
            out.at[origin], out.at[origin], send.at[1, k], recv.at[1, k], (ctx + 1 - 2 * core, exp)
        )
        copy.start()
        relayed.append(copy)
    flights[0].wait_recv()
    for copy in relayed:
        copy.wait_recv()
    for copy in flights + relayed:
        copy.wait_send()


def inputs_kernel(
    cache, fresh, res, ids, cache_out, fresh_out, res_out, ids_out,
    c_send, c_recv, f_send, f_recv, r_send, r_recv, i_send, i_recv, j_send, j_recv,
):
    chips, exp_count, ctx, exp, chip, core = place()
    ctx_count = 2 * chips
    id_flights = []
    for k in range(1, exp_count):
        copy = remote(
            ids, ids_out.at[ctx, exp], i_send.at[k], i_recv.at[k], (ctx, (exp + k) % exp_count)
        )
        copy.start()
        id_flights.append(copy)
    cache_flights = start_gather(cache, cache_out, c_send, c_recv)
    fresh_flights = start_gather(fresh, fresh_out, f_send, f_recv)
    res_flights = []
    for k in range(1, ctx_count):
        peer = (ctx + k) % ctx_count
        copy = remote(res.at[peer], res_out.at[ctx], r_send.at[k], r_recv.at[k], (peer, exp))
        copy.start()
        res_flights.append(copy)
    cache_out[ctx] = cache[...]
    fresh_out[ctx] = fresh[...]
    res_out[ctx] = res[ctx]
    ids_out[ctx, exp] = ids[...]
    for copy in id_flights:
        copy.wait()
    for k in range(1, ctx_count):
        copy = remote(
            ids_out.at[ctx],
            ids_out.at[ctx],
            j_send.at[k],
            j_recv.at[k],
            ((ctx + k) % ctx_count, exp),
        )
        copy.start()
        res_flights.append(copy)
    finish_gather(cache_out, cache_flights, c_send, c_recv)
    finish_gather(fresh_out, fresh_flights, f_send, f_recv)
    for copy in res_flights:
        copy.wait()


def heads_kernel(src, out, send, recv):
    _, _, ctx, _, _, _ = place()
    flights = start_gather(src, out, send, recv)
    out[ctx] = src[...]
    finish_gather(out, flights, send, recv)


def hidden_kernel(
    part, res, out, landed, a_send, a_recv, b_send, b_recv, x_send, x_recv, f_send, f_recv
):
    chips, exp_count, ctx, exp, chip, core = place()
    partner = ctx + 1 - 2 * core
    first = []
    for k in range(1, exp_count):
        peer = (exp + k) % exp_count
        copy = remote(part.at[peer], landed.at[k], a_send.at[k], a_recv.at[k], (ctx, peer))
        copy.start()
        first.append(copy)
    total = part[exp].astype(jnp.float32)
    for k in range(1, exp_count):
        first[k - 1].wait_recv()
        total = total + landed[k].astype(jnp.float32)
    out[ctx, exp] = (res[...].astype(jnp.float32) + total).astype(jnp.bfloat16)
    pending = []
    spread = [None]
    for k in range(1, exp_count):
        copy = remote(
            out.at[ctx, exp],
            out.at[ctx, exp],
            b_send.at[k],
            b_recv.at[k],
            (ctx, (exp + k) % exp_count),
        )
        copy.start()
        spread.append(copy)
    for k in range(exp_count):
        if k > 0:
            spread[k].wait_recv()
        source = (exp + exp_count - k) % exp_count
        block = out.at[ctx, source]
        row = []
        for p in range(chips):
            peer = partner if p == 0 else (chip + p) % chips * 2 + core
            copy = remote(block, block, x_send.at[p, k], x_recv.at[p, k], (peer, exp))
            copy.start()
            row.append(copy)
        pending.append(row)
    last = []
    for k in range(exp_count):
        source = (exp + exp_count - k) % exp_count
        for p in range(1, chips):
            pending[k][p].wait_recv()
            origin = (chip + chips - p) % chips * 2 + core
            block = out.at[origin, source]
            copy = remote(block, block, f_send.at[p, k], f_recv.at[p, k], (partner, exp))
            copy.start()
            last.append(copy)
    for row in pending:
        row[0].wait_recv()
    for copy in last:
        copy.wait()
    for copy in first + spread[1:] + [copy for row in pending for copy in row]:
        copy.wait_send()


def combine_kernel(
    y, hid, out, pair, cross_out, cross_in, home_out, home_in,
    p_send, p_recv, x_send, x_recv, e_send, e_recv,
):
    chips, exp_count, ctx, exp, chip, core = place()
    partner = ctx + 1 - 2 * core
    order = list(range(1, exp_count)) + [0]
    halves, crossing, homing = {}, {}, {}
    for k in order:
        dest = (exp + k) % exp_count
        for j in list(range(1, chips)) + [0]:
            theirs = (chip + j) % chips * 2 + 1 - core
            copy = remote(
                y.at[dest, theirs], pair.at[k, j], p_send.at[k, j], p_recv.at[k, j], (partner, exp)
            )
            copy.start()
            halves[k, j] = copy
    for k in order:
        dest = (exp + k) % exp_count
        for j in range(1, chips):
            owner = (chip + j) % chips * 2 + core
            halves[k, j].wait_recv()
            both = y[dest, owner].astype(jnp.float32) + pair[k, j].astype(jnp.float32)
            cross_out[k, j] = both.astype(jnp.bfloat16)
            copy = remote(
                cross_out.at[k, j],
                cross_in.at[k, j],
                x_send.at[k, j],
                x_recv.at[k, j],
                (owner, exp),
            )
            copy.start()
            crossing[k, j] = copy
    total = hid[...].astype(jnp.float32)
    for k in order:
        dest = (exp + k) % exp_count
        halves[k, 0].wait_recv()
        both = y[dest, ctx].astype(jnp.float32) + pair[k, 0].astype(jnp.float32)
        for j in range(1, chips):
            crossing[k, j].wait_recv()
            both = both + cross_in[k, j].astype(jnp.float32)
        if k == 0:
            total = total + both
        else:
            home_out[k] = both.astype(jnp.bfloat16)
            copy = remote(
                home_out.at[k], home_in.at[k], e_send.at[k], e_recv.at[k], (ctx, dest)
            )
            copy.start()
            homing[k] = copy
    for k in range(1, exp_count):
        homing[k].wait_recv()
        total = total + home_in[k].astype(jnp.float32)
    out[...] = total.astype(jnp.bfloat16)
    for copy in list(halves.values()) + list(crossing.values()) + list(homing.values()):
        copy.wait_send()


def exchange(kernel, shapes, scratch, *operands):
    vmem = pl.BlockSpec(memory_space=pltpu.VMEM)
    return pl.pallas_call(
        kernel,
        out_shape=shapes,
        in_specs=[vmem] * len(operands),
        out_specs=jax.tree.map(lambda _: vmem, shapes),
        scratch_shapes=scratch,
        compiler_params=pltpu.CompilerParams(
            has_side_effects=True, vmem_limit_bytes=VMEM_BYTES
        ),
    )(*operands)


def body(
    q_nope,
    q_rope,
    cache_keys,
    fresh_keys,
    block_order,
    w_uv,
    w_out,
    residual,
    norm_gain,
    router_weight,
    expert_ids,
    w_gate,
    w_up,
    w_down,
):
    ctx_count = lax.axis_size("ctx")
    exp_count = lax.axis_size("exp")
    ctx_index = lax.axis_index("ctx")
    exp_index = lax.axis_index("exp")
    rows_here, heads_here, latent_width = q_nope.shape
    value_width = w_uv.shape[2]
    key_width, cache_len = cache_keys.shape
    tok_here, model_width = residual.shape
    col_part = w_out.shape[1]
    chips = ctx_count // 2
    block_rows = rows_here * ctx_count // block_order.shape[0]
    dma = pltpu.SemaphoreType.DMA
    bf16 = functools.partial(jax.ShapeDtypeStruct, dtype=jnp.bfloat16)

    res_cols = residual.reshape(tok_here, ctx_count, col_part).transpose(1, 0, 2)
    cache_all, fresh_all, res_own, ids_all = exchange(
        inputs_kernel,
        (
            bf16((ctx_count, key_width, cache_len)),
            bf16((ctx_count, rows_here, key_width)),
            bf16((ctx_count, tok_here, col_part)),
            jax.ShapeDtypeStruct((ctx_count, exp_count) + expert_ids.shape, jnp.int32),
        ),
        [dma((2, chips))] * 4 + [dma((ctx_count,))] * 2 + [dma((exp_count,))] * 2
        + [dma((ctx_count,))] * 2,
        cache_keys, fresh_keys.T, res_cols, expert_ids,
    )
    cached = jnp.transpose(cache_all, (1, 0, 2)).reshape(key_width, ctx_count * cache_len)
    fresh = fresh_all.reshape(ctx_count * rows_here, key_width).T
    keys = jnp.concatenate([cached, fresh], axis=1)
    own_rows = ctx_index * rows_here + jnp.arange(rows_here, dtype=jnp.int32)
    own_pos = block_position(own_rows, block_order, block_rows)
    new_rows = jnp.arange(ctx_count * rows_here, dtype=jnp.int32)
    key_pos = jnp.concatenate(
        [
            jnp.full((ctx_count * cache_len,), -1, jnp.int32),
            block_position(new_rows, block_order, block_rows),
        ]
    )
    visible = key_pos[None, :] <= own_pos[:, None]
    row_max, row_sum, latent = attend(q_nope, q_rope, keys, visible)
    normal_lat = (latent / row_sum[:, :, None]).astype(jnp.bfloat16)
    head_out = jnp.einsum(
        "rhl,hlv->rhv", normal_lat, w_uv, preferred_element_type=jnp.float32
    ).astype(jnp.bfloat16).reshape(rows_here, heads_here * value_width)
    heads_all = exchange(
        heads_kernel,
        bf16((ctx_count,) + head_out.shape),
        [dma((2, chips))] * 2,
        head_out,
    )
    heads_all = (
        heads_all.reshape(ctx_count, exp_count, tok_here, -1)
        .transpose(1, 0, 2, 3)
        .reshape(exp_count * ctx_count * tok_here, -1)
    )
    head_partial = jnp.dot(heads_all, w_out, preferred_element_type=jnp.float32)
    group = ctx_count * tok_here
    hidden_all = exchange(
        hidden_kernel,
        bf16((ctx_count, exp_count, group, col_part)),
        [pltpu.VMEM((exp_count, group, col_part), jnp.bfloat16)]
        + [dma((exp_count,))] * 4
        + [dma((chips, exp_count))] * 4,
        head_partial.astype(jnp.bfloat16).reshape(exp_count, group, col_part),
        res_own.reshape(group, col_part),
    )
    tokens = exp_count * group
    hidden_rows = hidden_all.reshape(ctx_count, tokens, col_part).transpose(1, 0, 2)
    hidden_rows = hidden_rows.reshape(tokens, model_width)
    hidden = hidden_rows.astype(jnp.float32)
    mean_square = jnp.mean(hidden * hidden, axis=1, keepdims=True)
    normed = (hidden * lax.rsqrt(mean_square + NORM_EPS) * norm_gain).astype(jnp.bfloat16)
    affinity = jax.nn.sigmoid(jnp.dot(normed, router_weight, preferred_element_type=jnp.float32))
    expert_count = router_weight.shape[1]
    ids = ids_all.transpose(1, 0, 2, 3).reshape(tokens, -1)
    onehot = ids[:, :, None] == jnp.arange(expert_count, dtype=jnp.int32)[None, None, :]
    named = jnp.any(onehot, axis=1)
    chosen = jnp.where(named, affinity, 0.0)
    mixing = ROUTE_SCALE * chosen / jnp.sum(chosen, axis=1, keepdims=True)
    local_experts, _, hidden_units = w_gate.shape
    mine = lax.dynamic_slice_in_dim(mixing, exp_index * local_experts, local_experts, axis=1)
    acts = []
    for i in range(local_experts):
        gate = jnp.dot(normed, w_gate[i], preferred_element_type=jnp.float32)
        upward = jnp.dot(normed, w_up[i], preferred_element_type=jnp.float32)
        acts.append((jax.nn.silu(gate) * upward * mine[:, i : i + 1]).astype(jnp.bfloat16))
    acts = jnp.concatenate(acts, axis=1)
    down = w_down.reshape(local_experts * hidden_units, model_width)
    mixed = jnp.dot(acts, down, preferred_element_type=jnp.float32).astype(jnp.bfloat16)
    own_hidden = lax.dynamic_slice_in_dim(
        hidden_rows, (exp_index * ctx_count + ctx_index) * tok_here, tok_here, axis=0
    )
    block = (tok_here, model_width)
    return exchange(
        combine_kernel,
        bf16(block),
        [pltpu.VMEM((exp_count, chips) + block, jnp.bfloat16)] * 3
        + [pltpu.VMEM((exp_count,) + block, jnp.bfloat16)] * 2
        + [dma((exp_count, chips))] * 4
        + [dma((exp_count,))] * 2,
        mixed.reshape((exp_count, ctx_count) + block),
        own_hidden,
    )


def solution(mesh):
    return jax.shard_map(
        body,
        mesh=mesh,
        in_specs=(
            P("ctx", "exp", None),
            P("ctx", "exp"),
            P(None, "ctx"),
            P(None, "ctx"),
            P(),
            P("exp", None, None),
            P("exp", "ctx"),
            P(("ctx", "exp"), None),
            P(),
            P(),
            P(("ctx", "exp"), None),
            P("exp", None, "ctx"),
            P("exp", None, "ctx"),
            P("exp", "ctx", None),
        ),
        out_specs=P(("ctx", "exp"), None),
        check_vma=False,
    )
```

```python
import functools
import math

import jax
import jax.numpy as jnp
from jax import lax
from jax.experimental import pallas as pl
from jax.experimental.pallas import tpu as pltpu
from jax.sharding import PartitionSpec as P

QKD = 192
VMEM_BYTES = 56 * 1024 * 1024
SPARE_BYTES = 2 * 1024 * 1024

ROUTE_SCALE = 2.5
NORM_EPS = 1e-06


def block_position(row_index, block_order, block_rows):
    blocks = row_index // block_rows
    lookup = blocks[:, None] == jnp.arange(block_order.shape[0], dtype=jnp.int32)[None, :]
    leading = jnp.sum(jnp.where(lookup, block_order[None, :], 0), axis=1)
    return leading * block_rows + row_index % block_rows


def attend(query_lat, query_pe, keys, visible):
    row_count, head_count, latent_width = query_lat.shape
    key_count = keys.shape[1]
    pe_width = query_pe.shape[1] // head_count
    first_dot = jnp.dot(
        query_lat.reshape(row_count * head_count, latent_width),
        keys[:latent_width],
        preferred_element_type=jnp.float32,
    )
    second_dot = jnp.dot(
        query_pe.reshape(row_count * head_count, pe_width),
        keys[latent_width:],
        preferred_element_type=jnp.float32,
    )
    scores = ((first_dot + second_dot) * (1.0 / math.sqrt(QKD))).reshape(
        row_count, head_count, key_count
    )
    scores = jnp.where(visible[:, None, :], scores, -jnp.inf)
    row_max = jnp.max(scores, axis=2)
    exponent = jnp.exp(scores - row_max[:, :, None])
    row_sum = jnp.sum(exponent, axis=2)
    weights = exponent.astype(jnp.bfloat16).reshape(row_count * head_count, key_count)
    latent = lax.dot_general(
        weights, keys[:latent_width], (((1,), (1,)), ((), ())), preferred_element_type=jnp.float32
    )
    return (row_max, row_sum, latent.reshape(row_count, head_count, latent_width))


def remote(src, dst, send, recv, target):
    return pltpu.make_async_remote_copy(
        src_ref=src,
        dst_ref=dst,
        send_sem=send,
        recv_sem=recv,
        device_id=target,
        device_id_type=pl.DeviceIdType.MESH,
    )


def place():
    ctx_count, exp_count = lax.axis_size("ctx"), lax.axis_size("exp")
    ctx, exp = lax.axis_index("ctx"), lax.axis_index("exp")
    return ctx_count // 2, exp_count, ctx, exp, ctx // 2, ctx % 2


def greet(over_exp):
    ctx_count, exp_count = lax.axis_size("ctx"), lax.axis_size("exp")
    ctx, exp = lax.axis_index("ctx"), lax.axis_index("exp")
    barrier = pltpu.get_barrier_semaphore()
    peers = [((ctx + k) % ctx_count, exp) for k in range(1, ctx_count)]
    if over_exp:
        peers += [(ctx, (exp + k) % exp_count) for k in range(1, exp_count)]
    for peer in peers:
        pl.semaphore_signal(
            barrier, inc=1, device_id=peer, device_id_type=pl.DeviceIdType.MESH
        )
    pl.semaphore_wait(barrier, len(peers))


def column_block(rows, wide, ctx, exp, width):
    if not wide:
        return rows.at[ctx, exp]
    return rows.at[exp, :, pl.ds(pl.multiple_of(ctx * width, 128), width)]


def start_gather(src, out, send, recv):
    chips, _, ctx, exp, chip, core = place()
    flights = []
    for k in range(chips):
        peer = ctx + 1 - 2 * core if k == 0 else (chip + k) % chips * 2 + core
        copy = remote(src, out.at[ctx], send.at[0, k], recv.at[0, k], (peer, exp))
        copy.start()
        flights.append(copy)
    return flights


def finish_gather(out, flights, send, recv):
    chips, _, ctx, exp, chip, core = place()
    relayed = []
    for k in range(1, chips):
        flights[k].wait_recv()
        origin = (chip + chips - k) % chips * 2 + core
        copy = remote(
            out.at[origin], out.at[origin], send.at[1, k], recv.at[1, k], (ctx + 1 - 2 * core, exp)
        )
        copy.start()
        relayed.append(copy)
    flights[0].wait_recv()
    for copy in relayed:
        copy.wait_recv()
    for copy in flights + relayed:
        copy.wait_send()


def inputs_kernel(
    cache, fresh, res, ids, cache_out, fresh_out, res_out, ids_out,
    c_send, c_recv, f_send, f_recv, r_send, r_recv, i_send, i_recv, j_send, j_recv,
):
    chips, exp_count, ctx, exp, chip, core = place()
    ctx_count = 2 * chips
    greet(True)
    id_flights = []
    for k in range(1, exp_count):
        copy = remote(
            ids, ids_out.at[ctx, exp], i_send.at[k], i_recv.at[k], (ctx, (exp + k) % exp_count)
        )
        copy.start()
        id_flights.append(copy)
    cache_flights = start_gather(cache, cache_out, c_send, c_recv)
    fresh_flights = start_gather(fresh, fresh_out, f_send, f_recv)
    res_flights = []
    for k in range(1, ctx_count):
        peer = (ctx + k) % ctx_count
        copy = remote(res.at[peer], res_out.at[ctx], r_send.at[k], r_recv.at[k], (peer, exp))
        copy.start()
        res_flights.append(copy)
    cache_out[ctx] = cache[...]
    fresh_out[ctx] = fresh[...]
    res_out[ctx] = res[ctx]
    ids_out[ctx, exp] = ids[...]
    for copy in id_flights:
        copy.wait()
    for k in range(1, ctx_count):
        copy = remote(
            ids_out.at[ctx],
            ids_out.at[ctx],
            j_send.at[k],
            j_recv.at[k],
            ((ctx + k) % ctx_count, exp),
        )
        copy.start()
        res_flights.append(copy)
    finish_gather(cache_out, cache_flights, c_send, c_recv)
    finish_gather(fresh_out, fresh_flights, f_send, f_recv)
    for copy in res_flights:
        copy.wait()


def heads_kernel(src, out, send, recv):
    _, _, ctx, _, _, _ = place()
    greet(False)
    flights = start_gather(src, out, send, recv)
    out[ctx] = src[...]
    finish_gather(out, flights, send, recv)


def hidden_kernel(
    wide, part, res, out, landed, a_send, a_recv, b_send, b_recv, x_send, x_recv, f_send, f_recv
):
    chips, exp_count, ctx, exp, chip, core = place()
    partner = ctx + 1 - 2 * core
    width = part.shape[2]
    place_of = lambda c, e: column_block(out, wide, c, e, width)
    greet(True)
    first = []
    for k in range(1, exp_count):
        peer = (exp + k) % exp_count
        copy = remote(part.at[peer], landed.at[k], a_send.at[k], a_recv.at[k], (ctx, peer))
        copy.start()
        first.append(copy)
    total = part[exp].astype(jnp.float32)
    for k in range(1, exp_count):
        first[k - 1].wait_recv()
        total = total + landed[k].astype(jnp.float32)
    own = place_of(ctx, exp)
    own[...] = (res[...].astype(jnp.float32) + total).astype(jnp.bfloat16)
    pending = []
    spread = [None]
    for k in range(1, exp_count):
        copy = remote(
            own,
            own,
            b_send.at[k],
            b_recv.at[k],
            (ctx, (exp + k) % exp_count),
        )
        copy.start()
        spread.append(copy)
    for k in range(exp_count):
        if k > 0:
            spread[k].wait_recv()
        source = (exp + exp_count - k) % exp_count
        block = place_of(ctx, source)
        row = []
        for p in range(chips):
            peer = partner if p == 0 else (chip + p) % chips * 2 + core
            copy = remote(block, block, x_send.at[p, k], x_recv.at[p, k], (peer, exp))
            copy.start()
            row.append(copy)
        pending.append(row)
    last = []
    for k in range(exp_count):
        source = (exp + exp_count - k) % exp_count
        for p in range(1, chips):
            pending[k][p].wait_recv()
            origin = (chip + chips - p) % chips * 2 + core
            block = place_of(origin, source)
            copy = remote(block, block, f_send.at[p, k], f_recv.at[p, k], (partner, exp))
            copy.start()
            last.append(copy)
    for row in pending:
        row[0].wait_recv()
    for copy in last:
        copy.wait()
    for copy in first + spread[1:] + [copy for row in pending for copy in row]:
        copy.wait_send()


def combine_kernel(
    wide, y, hid, out, pair, cross_out, cross_in, home_out, home_in, final,
    p_send, p_recv, x_send, x_recv, e_send, e_recv, o_send, o_recv,
):
    chips, exp_count, ctx, exp, chip, core = place()
    partner = ctx + 1 - 2 * core
    ctx_count, tok, width = out.shape
    part_of = lambda c, e: column_block(y, wide, c, e, width)
    greet(True)
    order = list(range(1, exp_count)) + [0]
    halves, crossing, homing = {}, {}, {}
    for k in order:
        dest = (exp + k) % exp_count
        for j in list(range(1, chips)) + [0]:
            theirs = (chip + j) % chips * 2 + 1 - core
            copy = remote(
                part_of(theirs, dest),
                pair.at[k, j],
                p_send.at[k, j],
                p_recv.at[k, j],
                (partner, exp),
            )
            copy.start()
            halves[k, j] = copy
    for k in order:
        dest = (exp + k) % exp_count
        for j in range(1, chips):
            owner = (chip + j) % chips * 2 + core
            halves[k, j].wait_recv()
            both = part_of(owner, dest)[...].astype(jnp.float32) + pair[k, j].astype(jnp.float32)
            cross_out[k, j] = both.astype(jnp.bfloat16)
            copy = remote(
                cross_out.at[k, j],
                cross_in.at[k, j],
                x_send.at[k, j],
                x_recv.at[k, j],
                (owner, exp),
            )
            copy.start()
            crossing[k, j] = copy
    total = hid[...].astype(jnp.float32)
    for k in order:
        dest = (exp + k) % exp_count
        halves[k, 0].wait_recv()
        both = part_of(ctx, dest)[...].astype(jnp.float32) + pair[k, 0].astype(jnp.float32)
        for j in range(1, chips):
            crossing[k, j].wait_recv()
            both = both + cross_in[k, j].astype(jnp.float32)
        if k == 0:
            total = total + both
        else:
            home_out[k] = both.astype(jnp.bfloat16)
            copy = remote(
                home_out.at[k], home_in.at[k], e_send.at[k], e_recv.at[k], (ctx, dest)
            )
            copy.start()
            homing[k] = copy
    for k in range(1, exp_count):
        homing[k].wait_recv()
        total = total + home_in[k].astype(jnp.float32)
    for c in range(ctx_count):
        final[c] = total[c * tok : (c + 1) * tok].astype(jnp.bfloat16)
    last = []
    for k in range(1, ctx_count):
        peer = (ctx + k) % ctx_count
        copy = remote(final.at[peer], out.at[ctx], o_send.at[k], o_recv.at[k], (peer, exp))
        copy.start()
        last.append(copy)
    out[ctx] = final[ctx]
    for copy in last:
        copy.wait()
    for copy in list(halves.values()) + list(crossing.values()) + list(homing.values()):
        copy.wait_send()


def exchange(number, kernel, shapes, scratch, *operands):
    vmem = pl.BlockSpec(memory_space=pltpu.VMEM)
    held = jax.tree.leaves(shapes) + list(operands)
    held += [s for s in scratch if s.dtype == jnp.bfloat16]
    need = sum(2 * math.prod(h.shape) * h.dtype.itemsize for h in held) + SPARE_BYTES
    return pl.pallas_call(
        kernel,
        out_shape=shapes,
        in_specs=[vmem] * len(operands),
        out_specs=jax.tree.map(lambda _: vmem, shapes),
        scratch_shapes=scratch,
        compiler_params=pltpu.CompilerParams(
            collective_id=number, has_side_effects=True, vmem_limit_bytes=min(need, VMEM_BYTES)
        ),
    )(*operands)


def body(
    q_nope,
    q_rope,
    cache_keys,
    fresh_keys,
    block_order,
    w_uv,
    w_out,
    residual,
    norm_gain,
    router_weight,
    expert_ids,
    w_gate,
    w_up,
    w_down,
):
    ctx_count = lax.axis_size("ctx")
    exp_count = lax.axis_size("exp")
    ctx_index = lax.axis_index("ctx")
    exp_index = lax.axis_index("exp")
    rows_here, heads_here, latent_width = q_nope.shape
    value_width = w_uv.shape[2]
    key_width, cache_len = cache_keys.shape
    tok_here, model_width = residual.shape
    col_part = w_out.shape[1]
    chips = ctx_count // 2
    block_rows = rows_here * ctx_count // block_order.shape[0]
    dma = pltpu.SemaphoreType.DMA
    bf16 = functools.partial(jax.ShapeDtypeStruct, dtype=jnp.bfloat16)

    res_cols = residual.reshape(tok_here, ctx_count, col_part).transpose(1, 0, 2)
    cache_all, fresh_all, res_own, ids_all = exchange(
        0,
        inputs_kernel,
        (
            bf16((ctx_count, key_width, cache_len)),
            bf16((ctx_count, rows_here, key_width)),
            bf16((ctx_count, tok_here, col_part)),
            jax.ShapeDtypeStruct((ctx_count, exp_count) + expert_ids.shape, jnp.int32),
        ),
        [dma((2, chips))] * 4 + [dma((ctx_count,))] * 2 + [dma((exp_count,))] * 2
        + [dma((ctx_count,))] * 2,
        cache_keys, fresh_keys.T, res_cols, expert_ids,
    )
    cached = jnp.transpose(cache_all, (1, 0, 2)).reshape(key_width, ctx_count * cache_len)
    fresh = fresh_all.reshape(ctx_count * rows_here, key_width).T
    keys = jnp.concatenate([cached, fresh], axis=1)
    own_rows = ctx_index * rows_here + jnp.arange(rows_here, dtype=jnp.int32)
    own_pos = block_position(own_rows, block_order, block_rows)
    new_rows = jnp.arange(ctx_count * rows_here, dtype=jnp.int32)
    key_pos = jnp.concatenate(
        [
            jnp.full((ctx_count * cache_len,), -1, jnp.int32),
            block_position(new_rows, block_order, block_rows),
        ]
    )
    visible = key_pos[None, :] <= own_pos[:, None]
    row_max, row_sum, latent = attend(q_nope, q_rope, keys, visible)
    normal_lat = (latent / row_sum[:, :, None]).astype(jnp.bfloat16)
    head_out = jnp.einsum(
        "rhl,hlv->rhv", normal_lat, w_uv, preferred_element_type=jnp.float32
    ).astype(jnp.bfloat16).reshape(rows_here, heads_here * value_width)
    heads_all = exchange(
        1,
        heads_kernel,
        bf16((ctx_count,) + head_out.shape),
        [dma((2, chips))] * 2,
        head_out,
    )
    heads_all = (
        heads_all.reshape(ctx_count, exp_count, tok_here, -1)
        .transpose(1, 0, 2, 3)
        .reshape(exp_count * ctx_count * tok_here, -1)
    )
    head_partial = jnp.dot(heads_all, w_out, preferred_element_type=jnp.float32)
    group = ctx_count * tok_here
    wide = col_part % 128 == 0
    tokens = exp_count * group
    stripes = (exp_count, group, model_width)
    blocks = (ctx_count, exp_count, group, col_part)
    hidden_all = exchange(
        2,
        functools.partial(hidden_kernel, wide),
        bf16(stripes if wide else blocks),
        [pltpu.VMEM((exp_count, group, col_part), jnp.bfloat16)]
        + [dma((exp_count,))] * 4
        + [dma((chips, exp_count))] * 4,
        head_partial.astype(jnp.bfloat16).reshape(exp_count, group, col_part),
        res_own.reshape(group, col_part),
    )
    if not wide:
        hidden_all = hidden_all.transpose(1, 2, 0, 3)
    hidden_rows = hidden_all.reshape(tokens, model_width)
    hidden = hidden_rows.astype(jnp.float32)
    mean_square = jnp.mean(hidden * hidden, axis=1, keepdims=True)
    normed = (hidden * lax.rsqrt(mean_square + NORM_EPS) * norm_gain).astype(jnp.bfloat16)
    affinity = jax.nn.sigmoid(jnp.dot(normed, router_weight, preferred_element_type=jnp.float32))
    expert_count = router_weight.shape[1]
    ids = ids_all.transpose(1, 0, 2, 3).reshape(tokens, -1)
    onehot = ids[:, :, None] == jnp.arange(expert_count, dtype=jnp.int32)[None, None, :]
    named = jnp.any(onehot, axis=1)
    chosen = jnp.where(named, affinity, 0.0)
    mixing = ROUTE_SCALE * chosen / jnp.sum(chosen, axis=1, keepdims=True)
    local_experts, _, hidden_units = w_gate.shape
    mine = lax.dynamic_slice_in_dim(mixing, exp_index * local_experts, local_experts, axis=1)
    acts = []
    for i in range(local_experts):
        gate = jnp.dot(normed, w_gate[i], preferred_element_type=jnp.float32)
        upward = jnp.dot(normed, w_up[i], preferred_element_type=jnp.float32)
        acts.append((jax.nn.silu(gate) * upward * mine[:, i : i + 1]).astype(jnp.bfloat16))
    acts = jnp.concatenate(acts, axis=1)
    down = w_down.reshape(local_experts * hidden_units, model_width)
    mixed = jnp.dot(acts, down, preferred_element_type=jnp.float32).astype(jnp.bfloat16)
    own_hidden = lax.dynamic_slice(
        hidden_rows, (exp_index * group, ctx_index * col_part), (group, col_part)
    )
    mixed = mixed.reshape(stripes)
    if not wide:
        mixed = mixed.reshape(exp_count, group, ctx_count, col_part).transpose(2, 0, 1, 3)
    block = (group, col_part)
    owned = exchange(
        3,
        functools.partial(combine_kernel, wide),
        bf16((ctx_count, tok_here, col_part)),
        [pltpu.VMEM((exp_count, chips) + block, jnp.bfloat16)] * 3
        + [pltpu.VMEM((exp_count,) + block, jnp.bfloat16)] * 2
        + [pltpu.VMEM((ctx_count, tok_here, col_part), jnp.bfloat16)]
        + [dma((exp_count, chips))] * 4
        + [dma((exp_count,))] * 2
        + [dma((ctx_count,))] * 2,
        mixed,
        own_hidden,
    )
    return owned.transpose(1, 0, 2).reshape(tok_here, model_width)


def solution(mesh):
    return jax.shard_map(
        body,
        mesh=mesh,
        in_specs=(
            P("ctx", "exp", None),
            P("ctx", "exp"),
            P(None, "ctx"),
            P(None, "ctx"),
            P(),
            P("exp", None, None),
            P("exp", "ctx"),
            P(("ctx", "exp"), None),
            P(),
            P(),
            P(("ctx", "exp"), None),
            P("exp", None, "ctx"),
            P("exp", None, "ctx"),
            P("exp", "ctx", None),
        ),
        out_specs=P(("ctx", "exp"), None),
        check_vma=False,
    )
```
